64 devices in a mesh: rep: 8 (over x, y, core), dp: 8 (over z).
Axes of the slice: x: 2, y: 2, z: 8, core: 2. Of those that a mesh axis runs over, the one named last changes fastest.
The devices are a block of a 4x4x8 slice.
Arguments:
- a: bfloat16 [64, 4, 4096, 896], P(('rep', 'dp')), parts along dimension 0
- g: bfloat16 [64, 4, 4096, 2560], P(('rep', 'dp')), parts along dimension 0
Outputs:
- output: bfloat16 [32, 896, 2560], P('rep'), parts along dimension 0
There are 8 independent parts. The reference program is written for one: setup_inputs(seed, part) draws one part's arguments, and reference() takes and returns one part's arrays. A program takes and returns all parts, laid end to end along the dimension named above; each array names one.
All inputs are finite; a program needn't handle non-finite values.
Results may differ from the reference program's by a relative error of at most 0.012.
Values are sent between devices in bfloat16 or wider.
A program may use at most 768 MiB of HBM per device.

```python
import jax
import jax.numpy as jnp
from jax import lax

DEVICES = 8
MATRICES = 4
TOKENS = 4096
D = 896
FF = 2560


def setup_inputs(seed: int = 0, part: int = 0) -> dict:
    ka, kg, ks = (jax.random.fold_in(k, part) for k in jax.random.split(jax.random.key(seed), 3))
    size = 2.0 ** jax.random.uniform(ks, (DEVICES, MATRICES, 1, 1), jnp.float32, -1.0, 1.0)
    a = jax.random.normal(ka, (DEVICES, MATRICES, TOKENS, D), jnp.float32)
    g = size * jax.random.normal(kg, (DEVICES, MATRICES, TOKENS, FF), jnp.float32) * (DEVICES * TOKENS) ** -0.5
    return {"a": a.astype(jnp.bfloat16), "g": g.astype(jnp.bfloat16)}


def reference(a, g):
    def take(so_far, one):
        return so_far + jnp.einsum("ntd,ntf->ndf", *one, preferred_element_type=jnp.float32), None

    return lax.scan(take, jnp.zeros((MATRICES, D, FF), jnp.float32), (a, g))[0].astype(jnp.bfloat16)
```

```python
import functools

import jax
import jax.numpy as jnp
from jax import lax
from jax.experimental import pallas as pl
from jax.experimental.pallas import tpu as pltpu
from jax.sharding import PartitionSpec as P

COLS = 256
LANES = 128
A_SLOTS = 3
G_SLOTS = 3
P_SLOTS = 2
SEMS = 8


class Plan:
    def __init__(self, ring, matrices, tokens, rows, cols):
        self.ring, self.matrices, self.tokens, self.rows, self.cols = ring, matrices, tokens, rows, cols
        self.per_matrix = cols // COLS
        self.units = matrices * self.per_matrix
        self.sets = self.units // ring
        assert self.sets * ring == self.units and self.sets >= 3
        self.half = rows // 2
        self.span = -(-self.half // LANES) * LANES
        self.phase = 2 * (ring - 1)
        self.slots = self.sets * self.phase

    def final_slot(self, s):
        return (self.phase + 1 + 2 * s) if s < 2 else s * self.phase + 1

    def first_slot(self, s):
        return s if s < 2 else (s - 1) * self.phase

    def load_slot(self, m):
        last = (m - A_SLOTS + 1) * self.per_matrix - 1
        return self.final_slot(last // self.ring) + 1

    def need_slot(self, m):
        return self.first_slot(m * self.per_matrix // self.ring)

    def at(self, n):
        p, q = n // self.phase, n % self.phase
        b, k = q % 2, q // 2
        first, last = p == 0, p == self.sets - 1
        s_a = jnp.where(first, 0, jnp.where(last, self.sets - 2, p + 1))
        s_b = jnp.where(first, 1, jnp.where(last, self.sets - 1, p - 1))
        s = jnp.where(b == 0, s_a, s_b)
        scatter = jnp.logical_or(first, jnp.logical_and(b == 0, jnp.logical_not(last)))
        return s, k, scatter

    def final(self, n):
        ends, which = False, 0
        for s in range(self.sets):
            hit = n == self.final_slot(s)
            ends = jnp.logical_or(ends, hit)
            which = jnp.where(hit, s, which)
        return ends, which

    def job(self, n):
        s, k, scatter = self.at(n)
        ends, which = self.final(n)
        has = jnp.logical_and(jnp.logical_or(scatter, ends), n < self.slots)
        return has, jnp.where(ends, which, s), jnp.where(ends, self.ring - 1, k)


def reduce_kernel(plan, axis, a_ref, g_ref, x_ref, a_buf, g_buf, prod, a_sem, g_sem, send_sem, recv_sem):
    ring = plan.ring
    me = lax.axis_index(axis)
    neighbours = (lax.rem(me + 1, ring), lax.rem(me + ring - 1, ring))
    row0 = (0, plan.half)
    lane0 = (0, plan.rows - plan.span)

    barrier = pltpu.get_barrier_semaphore()
    for there in neighbours:
        pl.semaphore_signal(barrier, inc=1, device_id={axis: there}, device_id_type=pl.DeviceIdType.MESH)

    def chunk(d, k, scatter):
        hop = k + jnp.where(scatter, 1, 0)
        return lax.rem(me + (ring - hop if d == 0 else hop), ring)

    def job_unit(d, s, k):
        return s * ring + chunk(d, k, True)

    def block(u, d):
        return x_ref.at[u, pl.ds(row0[d], plan.half), :]

    def a_load(m):
        return pltpu.make_async_copy(a_ref.at[0, m], a_buf.at[m % A_SLOTS], a_sem.at[m % A_SLOTS])

    def g_load(d, u, n):
        m, j = u // plan.per_matrix, lax.rem(u, plan.per_matrix)
        slot = lax.rem(n, G_SLOTS)
        src = g_ref.at[0, m, :, pl.ds(pl.multiple_of(j * COLS, COLS), COLS)]
        return pltpu.make_async_copy(src, g_buf.at[d, slot], g_sem.at[d, slot])

    def fetch(n):
        has, s, k = plan.job(n)

        @pl.when(has)
        def _():
            for d in (0, 1):
                g_load(d, job_unit(d, s, k), n).start()

    def multiply(n):
        has, s, k = plan.job(n)

        @pl.when(has)
        def _():
            for d in (0, 1):
                u = job_unit(d, s, k)
                g_load(d, u, n).wait()
                prod[d, lax.rem(n, P_SLOTS)] = lax.dot_general(
                    a_buf[lax.rem(u // plan.per_matrix, A_SLOTS), :, pl.ds(lane0[d], plan.span)],
                    g_buf[d, lax.rem(n, G_SLOTS)],
                    (((0,), (0,)), ((), ())),
                    preferred_element_type=jnp.float32,
                )

    def add_product(d, n, u, fresh):
        off = row0[d] - lane0[d]
        mine = prod[d, lax.rem(n, P_SLOTS), pl.ds(off, plan.half), :]

        @pl.when(fresh)
        def _():
            x_ref[u, pl.ds(row0[d], plan.half), :] = mine.astype(x_ref.dtype)

        @pl.when(jnp.logical_not(fresh))
        def _():
            so_far = x_ref[u, pl.ds(row0[d], plan.half), :].astype(jnp.float32)
            x_ref[u, pl.ds(row0[d], plan.half), :] = (so_far + mine).astype(x_ref.dtype)

    def remote(d, u, n):
        i = lax.rem(n, SEMS)
        return pltpu.make_async_remote_copy(
            src_ref=block(u, d),
            dst_ref=block(u, d),
            send_sem=send_sem.at[d, i],
            recv_sem=recv_sem.at[d, i],
            device_id={axis: neighbours[d]},
            device_id_type=pl.DeviceIdType.MESH,
        )

    def turn(n):
        s, k, scatter = plan.at(n)
        has, js, jk = plan.job(n)
        for d in (0, 1):

            @pl.when(n >= 2)
            def _():
                remote(d, 0, n - 2 + SEMS).wait_recv()

            @pl.when(has)
            def _():
                add_product(d, n, job_unit(d, js, jk), jk == 0)

            @pl.when(n >= SEMS)
            def _():
                remote(d, 0, n).wait_send()

            remote(d, s * ring + chunk(d, k, scatter), n).start()

    first = range(min(A_SLOTS, plan.matrices))
    a_load(0).start()
    fetch(0)
    fetch(1)
    for m in first[1:]:
        a_load(m).start()
    fetch(2)
    a_load(0).wait()
    multiply(0)
    pl.semaphore_wait(barrier, 2)

    def body(n, _):
        turn(n)
        for m in range(1, plan.matrices):
            if m >= A_SLOTS:

                @pl.when(n == plan.load_slot(m))
                def _():
                    a_load(m).start()

            @pl.when(n + 1 == plan.need_slot(m))
            def _():
                a_load(m).wait()

        multiply(n + 1)
        fetch(n + 3)
        return 0

    lax.fori_loop(0, plan.slots, body, 0)
    for n in range(plan.slots - 2, plan.slots):
        for d in (0, 1):
            remote(d, 0, n).wait_recv()
    for n in range(plan.slots - SEMS, plan.slots):
        for d in (0, 1):
            remote(d, 0, n).wait_send()


def write_kernel(plan, x_ref, out_ref, sem):
    copies = []
    for u in range(plan.units):
        m, j = divmod(u, plan.per_matrix)
        copies.append(pltpu.make_async_copy(x_ref.at[u], out_ref.at[m, :, pl.ds(j * COLS, COLS)], sem.at[u]))
    for c in copies:
        c.start()
    for c in copies:
        c.wait()


def solution(mesh):
    axis = "dp"

    def device(a, g):
        _, matrices, tokens, rows = a.shape
        cols = g.shape[-1]
        plan = Plan(mesh.shape[axis], matrices, tokens, rows, cols)
        sums = pl.pallas_call(
            functools.partial(reduce_kernel, plan, axis),
            out_shape=pltpu.VMEM((plan.units, rows, COLS), jnp.bfloat16),
            in_specs=[pl.BlockSpec(memory_space=pl.ANY)] * 2,
            out_specs=pl.BlockSpec(memory_space=pltpu.VMEM),
            scratch_shapes=[
                pltpu.VMEM((A_SLOTS, tokens, rows), jnp.bfloat16),
                pltpu.VMEM((2, G_SLOTS, tokens, COLS), jnp.bfloat16),
                pltpu.VMEM((2, P_SLOTS, plan.span, COLS), jnp.float32),
                pltpu.SemaphoreType.DMA((A_SLOTS,)),
                pltpu.SemaphoreType.DMA((2, G_SLOTS)),
                pltpu.SemaphoreType.DMA((2, SEMS)),
                pltpu.SemaphoreType.DMA((2, SEMS)),
            ],
            compiler_params=pltpu.CompilerParams(
                collective_id=0, has_side_effects=True, vmem_limit_bytes=44 * 2**20
            ),
            name="ring_sums",
        )(a, g)
        return pl.pallas_call(
            functools.partial(write_kernel, plan),
            out_shape=jax.ShapeDtypeStruct((matrices, rows, cols), jnp.bfloat16),
            in_specs=[pl.BlockSpec(memory_space=pltpu.VMEM)],
            out_specs=pl.BlockSpec(memory_space=pl.ANY),
            scratch_shapes=[pltpu.SemaphoreType.DMA((plan.units,))],
            compiler_params=pltpu.CompilerParams(vmem_limit_bytes=2**20),
            name="write_sums",
        )(pltpu.with_memory_space_constraint(sums, pltpu.VMEM))

    spec = P(("rep", axis))
    return jax.shard_map(device, mesh=mesh, in_specs=(spec, spec), out_specs=P("rep"), check_vma=False)
```

```python
import functools

import jax
import jax.numpy as jnp
from jax import lax
from jax.experimental import pallas as pl
from jax.experimental.pallas import tpu as pltpu
from jax.sharding import PartitionSpec as P

COLS = 256
LANES = 128
A_SLOTS = 3
G_SLOTS = 3
PIECES = 4
P_SLOTS = 2
SEMS = 8
WRITES = 4


def dot(a, g):
    return lax.dot_general(a, g, (((0,), (0,)), ((), ())), preferred_element_type=jnp.float32)


class Plan:
    def __init__(self, ring, matrices, tokens, rows, cols):
        self.ring, self.matrices, self.tokens, self.rows, self.cols = ring, matrices, tokens, rows, cols
        self.per_matrix = cols // COLS
        self.units = matrices * self.per_matrix
        self.sets = self.units // ring
        assert self.sets * ring == self.units and self.sets >= 3
        self.half = rows // 2
        self.span = -(-self.half // LANES) * LANES
        self.phase = 2 * (ring - 1)
        self.slots = self.sets * self.phase

    def final_slot(self, s):
        return (self.phase + 1 + 2 * s) if s < 2 else s * self.phase + 1

    def first_slot(self, s):
        return s if s < 2 else (s - 1) * self.phase

    def load_slot(self, m):
        if m < A_SLOTS:
            return m
        last = (m - A_SLOTS + 1) * self.per_matrix - 1
        return self.final_slot(last // self.ring) + 1

    def need_slot(self, m):
        return self.first_slot(m * self.per_matrix // self.ring)

    def at(self, n):
        p, q = n // self.phase, n % self.phase
        b, k = q % 2, q // 2
        first, last = p == 0, p == self.sets - 1
        s_a = jnp.where(first, 0, jnp.where(last, self.sets - 2, p + 1))
        s_b = jnp.where(first, 1, jnp.where(last, self.sets - 1, p - 1))
        s = jnp.where(b == 0, s_a, s_b)
        scatter = jnp.logical_or(first, jnp.logical_and(b == 0, jnp.logical_not(last)))
        return s, k, scatter

    def final(self, n):
        ends, which = False, 0
        for s in range(self.sets):
            hit = n == self.final_slot(s)
            ends = jnp.logical_or(ends, hit)
            which = jnp.where(hit, s, which)
        return ends, which

    def job(self, n):
        s, k, scatter = self.at(n)
        ends, which = self.final(n)
        has = jnp.logical_and(jnp.logical_or(scatter, ends), n < self.slots)
        return has, jnp.where(ends, which, s), jnp.where(ends, self.ring - 1, k)


def reduce_kernel(plan, axis, a_ref, g_ref, x_ref, a_buf, g_buf, prod, a_sem, g_sem, send_sem, recv_sem, first_sem):
    ring = plan.ring
    me = lax.axis_index(axis)
    neighbours = (lax.rem(me + 1, ring), lax.rem(me + ring - 1, ring))
    row0 = (0, plan.half)
    lane0 = (0, plan.rows - plan.span)

    barrier = pltpu.get_barrier_semaphore()
    for there in neighbours:
        pl.semaphore_signal(barrier, inc=1, device_id={axis: there}, device_id_type=pl.DeviceIdType.MESH)

    def chunk(d, k, scatter):
        hop = k + jnp.where(scatter, 1, 0)
        return lax.rem(me + (ring - hop if d == 0 else ring - 2 + hop), ring)

    def shared(k):
        return lax.rem(2 * k, ring) == 0

    def job_unit(d, s, k):
        return s * ring + chunk(d, k, True)

    def columns(u):
        j = lax.rem(u, plan.per_matrix)
        return u // plan.per_matrix, pl.ds(pl.multiple_of(j * COLS, COLS), COLS)

    def block(u, d):
        m, cols = columns(u)
        return x_ref.at[m, pl.ds(row0[d], plan.half), cols]

    def a_load(m):
        return pltpu.make_async_copy(a_ref.at[0, m], a_buf.at[m % A_SLOTS], a_sem.at[m % A_SLOTS])

    def g_load(d, u, n):
        m, cols = columns(u)
        slot = lax.rem(n, G_SLOTS)
        return pltpu.make_async_copy(g_ref.at[0, m, :, cols], g_buf.at[d, slot], g_sem.at[d, slot])

    def fetch(n):
        has, s, k = plan.job(n)

        @pl.when(has)
        def _():
            g_load(0, job_unit(0, s, k), n).start()

        @pl.when(jnp.logical_and(has, jnp.logical_not(shared(k))))
        def _():
            g_load(1, job_unit(1, s, k), n).start()

    def multiply(n):
        has, s, k = plan.job(n)

        @pl.when(has)
        def _():
            for d in (0, 1):
                u = job_unit(d, s, k)
                if d == 0:
                    g_load(0, u, n).wait()
                else:

                    @pl.when(jnp.logical_not(shared(k)))
                    def _():
                        g_load(1, u, n).wait()

                from_buf = 0 if d == 0 else jnp.where(shared(k), 0, 1)
                prod[d, lax.rem(n, P_SLOTS)] = dot(
                    a_buf[lax.rem(u // plan.per_matrix, A_SLOTS), :, pl.ds(lane0[d], plan.span)],
                    g_buf[from_buf, lax.rem(n, G_SLOTS)],
                )

    piece = plan.tokens // PIECES
    splits = ((0, plan.span), (plan.span, plan.rows - plan.span))

    def first_a(d, i):
        toks, lanes = pl.ds(i * piece, piece), pl.ds(*splits[d])
        return pltpu.make_async_copy(a_ref.at[0, 0, toks, lanes], a_buf.at[0, toks, lanes], first_sem.at[d, i])

    def first_g(i):
        toks, (m, cols) = pl.ds(i * piece, piece), columns(job_unit(0, 0, 0))
        return pltpu.make_async_copy(g_ref.at[0, m, toks, cols], g_buf.at[0, 0, toks], first_sem.at[2, i])

    def first_product(d):
        for i in range(PIECES):
            first_a(d, i).wait()
            if d == 0:
                first_g(i).wait()
            toks = pl.ds(i * piece, piece)
            part = dot(a_buf[0, toks, pl.ds(lane0[d], plan.span)], g_buf[0, 0, toks])
            if i == 0:
                prod[d, 0] = part
            else:
                prod[d, 0] += part

    def add_product(d, n, u, fresh):
        off = row0[d] - lane0[d]
        mine = prod[d, lax.rem(n, P_SLOTS), pl.ds(off, plan.half), :]
        m, cols = columns(u)
        there = (m, pl.ds(row0[d], plan.half), cols)

        if fresh is True:
            x_ref[there] = mine.astype(x_ref.dtype)
            return

        @pl.when(fresh)
        def _():
            x_ref[there] = mine.astype(x_ref.dtype)

        @pl.when(jnp.logical_not(fresh))
        def _():
            x_ref[there] = (x_ref[there].astype(jnp.float32) + mine).astype(x_ref.dtype)

    def remote(d, u, n):
        i = lax.rem(n, SEMS)
        return pltpu.make_async_remote_copy(
            src_ref=block(u, d),
            dst_ref=block(u, d),
            send_sem=send_sem.at[d, i],
            recv_sem=recv_sem.at[d, i],
            device_id={axis: neighbours[d]},
            device_id_type=pl.DeviceIdType.MESH,
        )

    def turn_one(d, n):
        s, k, scatter = plan.at(n)
        has, js, jk = plan.job(n)

        @pl.when(n >= 2)
        def _():
            remote(d, 0, n - 2 + SEMS).wait_recv()

        @pl.when(has)
        def _():
            add_product(d, n, job_unit(d, js, jk), jk == 0)

        @pl.when(n >= SEMS)
        def _():
            remote(d, 0, n).wait_send()

        remote(d, s * ring + chunk(d, k, scatter), n).start()

    def first_turn(d):
        u = job_unit(d, 0, 0)
        add_product(d, 0, u, True)
        remote(d, u, 0).start()

    def multiply_next(n):
        for m in range(1, plan.matrices):
            if m >= 2:

                @pl.when(n == plan.load_slot(m))
                def _():
                    a_load(m).start()

            @pl.when(n + 1 == plan.need_slot(m))
            def _():
                a_load(m).wait()

        multiply(n + 1)

    for i in range(PIECES):
        first_a(0, i).start()
        first_g(i).start()
    for i in range(PIECES):
        first_a(1, i).start()
    fetch(1)
    if plan.matrices > 1:
        a_load(1).start()
    first_product(0)
    pl.semaphore_wait(barrier, 2)
    first_turn(0)
    first_product(1)
    first_turn(1)
    fetch(2)
    multiply_next(0)
    fetch(3)

    def body(n, _):
        for d in (0, 1):
            turn_one(d, n)
        multiply_next(n)
        fetch(n + 3)
        return 0

    lax.fori_loop(1, plan.slots, body, 0)
    for n in range(plan.slots - 2, plan.slots):
        for d in (0, 1):
            remote(d, 0, n).wait_recv()
    for n in range(plan.slots - SEMS, plan.slots):
        for d in (0, 1):
            remote(d, 0, n).wait_send()


def write_kernel(pieces, x_ref, out_ref, sem):
    matrices, rows, _ = x_ref.shape
    tall = rows // pieces
    copies = []
    for i in range(matrices * pieces):
        at = (i // pieces, pl.ds(i % pieces * tall, tall))
        copies.append(pltpu.make_async_copy(x_ref.at[at], out_ref.at[at], sem.at[i]))
    for c in copies:
        c.start()
    for c in copies:
        c.wait()


def solution(mesh):
    axis = "dp"

    def device(a, g):
        _, matrices, tokens, rows = a.shape
        cols = g.shape[-1]
        plan = Plan(mesh.shape[axis], matrices, tokens, rows, cols)
        sums = pl.pallas_call(
            functools.partial(reduce_kernel, plan, axis),
            out_shape=pltpu.VMEM((matrices, rows, cols), jnp.bfloat16),
            in_specs=[pl.BlockSpec(memory_space=pl.ANY)] * 2,
            out_specs=pl.BlockSpec(memory_space=pltpu.VMEM),
            scratch_shapes=[
                pltpu.VMEM((A_SLOTS, tokens, rows), jnp.bfloat16),
                pltpu.VMEM((2, G_SLOTS, tokens, COLS), jnp.bfloat16),
                pltpu.VMEM((2, P_SLOTS, plan.span, COLS), jnp.float32),
                pltpu.SemaphoreType.DMA((A_SLOTS,)),
                pltpu.SemaphoreType.DMA((2, G_SLOTS)),
                pltpu.SemaphoreType.DMA((2, SEMS)),
                pltpu.SemaphoreType.DMA((2, SEMS)),
                pltpu.SemaphoreType.DMA((3, PIECES)),
            ],
            compiler_params=pltpu.CompilerParams(
                collective_id=0, has_side_effects=True, vmem_limit_bytes=44 * 2**20
            ),
            name="ring_sums",
        )(a, g)
        return pl.pallas_call(
            functools.partial(write_kernel, WRITES),
            out_shape=jax.ShapeDtypeStruct((matrices, rows, cols), jnp.bfloat16),
            in_specs=[pl.BlockSpec(memory_space=pltpu.VMEM)],
            out_specs=pl.BlockSpec(memory_space=pl.ANY),
            scratch_shapes=[pltpu.SemaphoreType.DMA((matrices * WRITES,))],
            compiler_params=pltpu.CompilerParams(vmem_limit_bytes=2**20),
            name="write_sums",
        )(pltpu.with_memory_space_constraint(sums, pltpu.VMEM))

    spec = P(("rep", axis))
    return jax.shard_map(device, mesh=mesh, in_specs=(spec, spec), out_specs=P("rep"), check_vma=False)
```

```python
import functools

import jax
import jax.numpy as jnp
from jax import lax
from jax.experimental import pallas as pl
from jax.experimental.pallas import tpu as pltpu
from jax.sharding import PartitionSpec as P

COLS = 256
LANES = 128
A_SLOTS = 3
G_SLOTS = 3
PIECES = 4
P_SLOTS = 2
SEMS = 8
WRITES = 4


def dot(a, g):
    return lax.dot_general(a, g, (((0,), (0,)), ((), ())), preferred_element_type=jnp.float32)


class Plan:
    def __init__(self, ring, matrices, tokens, rows, cols):
        self.ring, self.matrices, self.tokens, self.rows, self.cols = ring, matrices, tokens, rows, cols
        self.per_matrix = cols // COLS
        self.units = matrices * self.per_matrix
        self.sets = self.units // ring
        assert self.sets * ring == self.units and self.sets >= 3
        assert matrices >= 2 and self.per_matrix % 2 == 0 and self.per_matrix >= ring > self.per_matrix // 2
        self.half = rows // 2
        self.quick = -(-self.half // (2 * LANES)) * LANES
        self.span = -(-self.half // LANES) * LANES
        self.phase = 2 * (ring - 1)
        self.slots = self.sets * self.phase

    def unit(self, s, c):
        h = self.per_matrix // 2
        pair = jnp.where(c < h, c + h * s, self.per_matrix + c - h + (self.ring - h) * s)
        return jnp.where(s < 2, pair, s * self.ring + c)

    def final_slot(self, s):
        return (self.phase + 1 + 2 * s) if s < 2 else s * self.phase + 1

    def first_slot(self, s):
        return s if s < 2 else (s - 1) * self.phase

    def load_slot(self, m):
        if m < A_SLOTS:
            return m
        last = (m - A_SLOTS + 1) * self.per_matrix - 1
        return self.final_slot(max(last // self.ring, 1)) + 1

    def need_slot(self, m):
        return self.first_slot(m * self.per_matrix // self.ring)

    def columns(self, u):
        j = lax.rem(u, self.per_matrix)
        return u // self.per_matrix, pl.ds(pl.multiple_of(j * COLS, COLS), COLS)

    def chunk(self, me, d, hop):
        return lax.rem(me + (self.ring - hop if d == 0 else self.ring - 2 + hop), self.ring)

    def at(self, n):
        p, q = n // self.phase, n % self.phase
        b, k = q % 2, q // 2
        first, last = p == 0, p == self.sets - 1
        s_a = jnp.where(first, 0, jnp.where(last, self.sets - 2, p + 1))
        s_b = jnp.where(first, 1, jnp.where(last, self.sets - 1, p - 1))
        s = jnp.where(b == 0, s_a, s_b)
        scatter = jnp.logical_or(first, jnp.logical_and(b == 0, jnp.logical_not(last)))
        return s, k, scatter

    def final(self, n):
        ends, which = False, 0
        for s in range(self.sets):
            hit = n == self.final_slot(s)
            ends = jnp.logical_or(ends, hit)
            which = jnp.where(hit, s, which)
        return ends, which

    def job(self, n):
        s, k, scatter = self.at(n)
        ends, which = self.final(n)
        has = jnp.logical_and(jnp.logical_or(scatter, ends), n < self.slots)
        return has, jnp.where(ends, which, s), jnp.where(ends, self.ring - 1, k)


def reduce_kernel(plan, axis, a_ref, g_ref, x_ref, a_buf, g_buf, prod, a_sem, g_sem, send_sem, recv_sem, first_sem, first_send, first_recv):
    ring = plan.ring
    me = lax.axis_index(axis)
    neighbours = (lax.rem(me + 1, ring), lax.rem(me + ring - 1, ring))
    row0 = (0, plan.half)
    lane0 = (0, plan.rows - plan.span)

    barrier = pltpu.get_barrier_semaphore()
    for there in neighbours:
        pl.semaphore_signal(barrier, inc=1, device_id={axis: there}, device_id_type=pl.DeviceIdType.MESH)

    def chunk(d, k, scatter):
        return plan.chunk(me, d, k + jnp.where(scatter, 1, 0))

    def shared(k):
        return lax.rem(2 * k, ring) == 0

    def job_unit(d, s, k):
        return plan.unit(s, chunk(d, k, True))

    columns = plan.columns

    def block(u, d):
        m, cols = columns(u)
        return x_ref.at[m, pl.ds(row0[d], plan.half), cols]

    def a_load(m):
        return pltpu.make_async_copy(a_ref.at[0, m], a_buf.at[m % A_SLOTS], a_sem.at[m % A_SLOTS])

    def g_load(d, u, n):
        m, cols = columns(u)
        slot = lax.rem(n, G_SLOTS)
        return pltpu.make_async_copy(g_ref.at[0, m, :, cols], g_buf.at[d, slot], g_sem.at[d, slot])

    def fetch(n):
        has, s, k = plan.job(n)

        @pl.when(has)
        def _():
            g_load(0, job_unit(0, s, k), n).start()

        @pl.when(jnp.logical_and(has, jnp.logical_not(shared(k))))
        def _():
            g_load(1, job_unit(1, s, k), n).start()

    def multiply(n):
        has, s, k = plan.job(n)

        @pl.when(has)
        def _():
            for d in (0, 1):
                u = job_unit(d, s, k)
                if d == 0:
                    g_load(0, u, n).wait()
                else:

                    @pl.when(jnp.logical_not(shared(k)))
                    def _():
                        g_load(1, u, n).wait()

                from_buf = 0 if d == 0 else jnp.where(shared(k), 0, 1)
                prod[d, lax.rem(n, P_SLOTS)] = dot(
                    a_buf[lax.rem(u // plan.per_matrix, A_SLOTS), :, pl.ds(lane0[d], plan.span)],
                    g_buf[from_buf, lax.rem(n, G_SLOTS)],
                )

    piece, quick = plan.tokens // PIECES, plan.quick
    first_unit = job_unit(0, 0, 0)
    first_m = first_unit // plan.per_matrix
    other_m = 1 - first_m
    parts = (
        (0, (0, quick), (0, quick), (0, quick)),
        (1, (plan.half - quick, quick), (plan.span - quick, quick), (plan.rows - quick, quick)),
        (0, (quick, plan.half - quick), (quick, plan.span - quick), (quick, plan.span - quick)),
        (1, (0, plan.half - quick), (0, plan.span - quick), (plan.span, plan.rows - quick - plan.span)),
    )

    def first_a(p, i):
        toks, lanes = pl.ds(i * piece, piece), pl.ds(*parts[p][3])
        return pltpu.make_async_copy(
            a_ref.at[0, first_m, toks, lanes], a_buf.at[first_m, toks, lanes], first_sem.at[p, i]
        )

    def first_g(i):
        toks, (m, cols) = pl.ds(i * piece, piece), columns(first_unit)
        return pltpu.make_async_copy(g_ref.at[0, m, toks, cols], g_buf.at[0, 0, toks], first_sem.at[len(parts), i])

    def first_remote(p):
        d, (row, tall), _, _ = parts[p]
        m, cols = columns(first_unit)
        at = x_ref.at[m, pl.ds(row0[d] + row, tall), cols]
        return pltpu.make_async_remote_copy(
            src_ref=at,
            dst_ref=at,
            send_sem=first_send.at[p],
            recv_sem=first_recv.at[p],
            device_id={axis: neighbours[d]},
            device_id_type=pl.DeviceIdType.MESH,
        )

    def first_part(p):
        d, (row, tall), (at, wide), _ = parts[p]
        for i in range(PIECES):
            first_a(p, i).wait()
            if p == 0:
                first_g(i).wait()
            toks = pl.ds(i * piece, piece)
            made = dot(a_buf[first_m, toks, pl.ds(lane0[d] + at, wide)], g_buf[0, 0, toks])
            if i == 0:
                prod[d, 0, pl.ds(at, wide), :] = made
            else:
                prod[d, 0, pl.ds(at, wide), :] += made
        m, cols = columns(first_unit)
        mine = prod[d, 0, pl.ds(row0[d] - lane0[d] + row, tall), :]
        x_ref[m, pl.ds(row0[d] + row, tall), cols] = mine.astype(x_ref.dtype)
        if p == 0:
            pl.semaphore_wait(barrier, 2)
        first_remote(p).start()

    other_a = pltpu.make_async_copy(a_ref.at[0, other_m], a_buf.at[other_m], a_sem.at[1])

    def add_product(d, n, u, fresh):
        off = row0[d] - lane0[d]
        mine = prod[d, lax.rem(n, P_SLOTS), pl.ds(off, plan.half), :]
        m, cols = columns(u)
        there = (m, pl.ds(row0[d], plan.half), cols)

        @pl.when(fresh)
        def _():
            x_ref[there] = mine.astype(x_ref.dtype)

        @pl.when(jnp.logical_not(fresh))
        def _():
            x_ref[there] = (x_ref[there].astype(jnp.float32) + mine).astype(x_ref.dtype)

    def remote(d, u, n):
        i = lax.rem(n, SEMS)
        return pltpu.make_async_remote_copy(
            src_ref=block(u, d),
            dst_ref=block(u, d),
            send_sem=send_sem.at[d, i],
            recv_sem=recv_sem.at[d, i],
            device_id={axis: neighbours[d]},
            device_id_type=pl.DeviceIdType.MESH,
        )

    def turn_one(d, n):
        s, k, scatter = plan.at(n)
        has, js, jk = plan.job(n)
        mine = [p for p in range(len(parts)) if parts[p][0] == d]

        @pl.when(n == 2)
        def _():
            for p in mine:
                first_remote(p).wait_recv()

        @pl.when(n > 2)
        def _():
            remote(d, 0, n - 2 + SEMS).wait_recv()

        @pl.when(has)
        def _():
            add_product(d, n, job_unit(d, js, jk), jk == 0)

        @pl.when(n == SEMS)
        def _():
            for p in mine:
                first_remote(p).wait_send()

        @pl.when(n > SEMS)
        def _():
            remote(d, 0, n).wait_send()

        remote(d, plan.unit(s, chunk(d, k, scatter)), n).start()

    def multiply_next(n):
        @pl.when(n == 1)
        def _():
            other_a.wait()

        for m in range(2, plan.matrices):

            @pl.when(n == plan.load_slot(m))
            def _():
                a_load(m).start()

            @pl.when(n + 1 == plan.need_slot(m))
            def _():
                a_load(m).wait()

        multiply(n + 1)

    for p in range(len(parts)):
        for i in range(PIECES):
            first_a(p, i).start()
            if p == 0:
                first_g(i).start()
    fetch(1)
    other_a.start()
    for p in range(len(parts)):
        first_part(p)
    fetch(2)
    multiply_next(0)
    fetch(3)

    def body(n, _):
        for d in (0, 1):
            turn_one(d, n)
        multiply_next(n)
        fetch(n + 3)
        return 0

    slots = plan.slots
    lax.fori_loop(1, slots, body, 0)
    for n in range(slots - 2, slots):
        for d in (0, 1):
            remote(d, 0, n).wait_recv()
    for n in range(slots - SEMS, slots):
        for d in (0, 1):
            remote(d, 0, n).wait_send()


def write_kernel(pieces, x_ref, out_ref, sem):
    matrices, rows, _ = x_ref.shape
    tall = rows // pieces
    copies = []
    for i in range(matrices * pieces):
        at = (i // pieces, pl.ds(i % pieces * tall, tall))
        copies.append(pltpu.make_async_copy(x_ref.at[at], out_ref.at[at], sem.at[i]))
    for c in copies:
        c.start()
    for c in copies:
        c.wait()


def solution(mesh):
    axis = "dp"

    def device(a, g):
        _, matrices, tokens, rows = a.shape
        cols = g.shape[-1]
        plan = Plan(mesh.shape[axis], matrices, tokens, rows, cols)
        sums = pl.pallas_call(
            functools.partial(reduce_kernel, plan, axis),
            out_shape=pltpu.VMEM((matrices, rows, cols), jnp.bfloat16),
            in_specs=[pl.BlockSpec(memory_space=pl.ANY)] * 2,
            out_specs=pl.BlockSpec(memory_space=pltpu.VMEM),
            scratch_shapes=[
                pltpu.VMEM((A_SLOTS, tokens, rows), jnp.bfloat16),
                pltpu.VMEM((2, G_SLOTS, tokens, COLS), jnp.bfloat16),
                pltpu.VMEM((2, P_SLOTS, plan.span, COLS), jnp.float32),
                pltpu.SemaphoreType.DMA((A_SLOTS,)),
                pltpu.SemaphoreType.DMA((2, G_SLOTS)),
                pltpu.SemaphoreType.DMA((2, SEMS)),
                pltpu.SemaphoreType.DMA((2, SEMS)),
                pltpu.SemaphoreType.DMA((5, PIECES)),
                pltpu.SemaphoreType.DMA((4,)),
                pltpu.SemaphoreType.DMA((4,)),
            ],
            compiler_params=pltpu.CompilerParams(
                collective_id=0, has_side_effects=True, vmem_limit_bytes=44 * 2**20
            ),
            name="ring_sums",
        )(a, g)
        return pl.pallas_call(
            functools.partial(write_kernel, WRITES),
            out_shape=jax.ShapeDtypeStruct((matrices, rows, cols), jnp.bfloat16),
            in_specs=[pl.BlockSpec(memory_space=pltpu.VMEM)],
            out_specs=pl.BlockSpec(memory_space=pl.ANY),
            scratch_shapes=[pltpu.SemaphoreType.DMA((matrices * WRITES,))],
            compiler_params=pltpu.CompilerParams(vmem_limit_bytes=2**20),
            name="write_sums",
        )(pltpu.with_memory_space_constraint(sums, pltpu.VMEM))

    spec = P(("rep", axis))
    return jax.shard_map(device, mesh=mesh, in_specs=(spec, spec), out_specs=P("rep"), check_vma=False)
```

```python
import functools

import jax
import jax.numpy as jnp
from jax import lax
from jax.experimental import pallas as pl
from jax.experimental.pallas import tpu as pltpu
from jax.sharding import PartitionSpec as P

COLS = 256
LANES = 128
A_SLOTS = 3
G_SLOTS = 3
PIECES = 4
P_SLOTS = 2
SEMS = 8
WRITES = 4


def dot(a, g):
    return lax.dot_general(a, g, (((0,), (0,)), ((), ())), preferred_element_type=jnp.float32)


class Plan:
    def __init__(self, ring, matrices, tokens, rows, cols):
        self.ring, self.matrices, self.tokens, self.rows, self.cols = ring, matrices, tokens, rows, cols
        self.per_matrix = cols // COLS
        self.units = matrices * self.per_matrix
        self.sets = self.units // ring
        assert self.sets * ring == self.units and self.sets >= 3
        assert matrices >= 2 and self.per_matrix % 2 == 0 and self.per_matrix >= ring > self.per_matrix // 2
        self.half = rows // 2
        self.quick = -(-self.half // (2 * LANES)) * LANES
        self.span = -(-self.half // LANES) * LANES
        self.phase = 2 * (ring - 1)
        self.slots = self.sets * self.phase
        self.cut = self.slots - 1

    def unit(self, s, c):
        h = self.per_matrix // 2
        pair = jnp.where(c < h, c + h * s, self.per_matrix + c - h + (self.ring - h) * s)
        return jnp.where(s < 2, pair, s * self.ring + c)

    def columns(self, u):
        j = lax.rem(u, self.per_matrix)
        return u // self.per_matrix, pl.ds(pl.multiple_of(j * COLS, COLS), COLS)

    def chunk(self, me, d, hop):
        return lax.rem(me + (self.ring - hop if d == 0 else self.ring - 2 + hop), self.ring)

    def final_slot(self, s):
        return (self.phase + 1 + 2 * s) if s < 2 else s * self.phase + 1

    def first_slot(self, s):
        return s if s < 2 else (s - 1) * self.phase

    def load_slot(self, m):
        if m < A_SLOTS:
            return m
        last = (m - A_SLOTS + 1) * self.per_matrix - 1
        return self.final_slot(max(last // self.ring, 1)) + 1

    def need_slot(self, m):
        return self.first_slot(m * self.per_matrix // self.ring)

    def columns(self, u):
        j = lax.rem(u, self.per_matrix)
        return u // self.per_matrix, pl.ds(pl.multiple_of(j * COLS, COLS), COLS)

    def chunk(self, me, d, hop):
        return lax.rem(me + (self.ring - hop if d == 0 else self.ring - 2 + hop), self.ring)

    def at(self, n):
        p, q = n // self.phase, n % self.phase
        b, k = q % 2, q // 2
        first, last = p == 0, p == self.sets - 1
        s_a = jnp.where(first, 0, jnp.where(last, self.sets - 2, p + 1))
        s_b = jnp.where(first, 1, jnp.where(last, self.sets - 1, p - 1))
        s = jnp.where(b == 0, s_a, s_b)
        scatter = jnp.logical_or(first, jnp.logical_and(b == 0, jnp.logical_not(last)))
        return s, k, scatter

    def final(self, n):
        ends, which = False, 0
        for s in range(self.sets):
            hit = n == self.final_slot(s)
            ends = jnp.logical_or(ends, hit)
            which = jnp.where(hit, s, which)
        return ends, which

    def job(self, n):
        s, k, scatter = self.at(n)
        ends, which = self.final(n)
        has = jnp.logical_and(jnp.logical_or(scatter, ends), n < self.slots)
        return has, jnp.where(ends, which, s), jnp.where(ends, self.ring - 1, k)


def reduce_kernel(plan, axis, a_ref, g_ref, x_ref, r_ref, l_ref, a_buf, g_buf, prod, a_sem, g_sem, send_sem, recv_sem, first_sem, first_send, first_recv):
    ring = plan.ring
    me = lax.axis_index(axis)
    neighbours = (lax.rem(me + 1, ring), lax.rem(me + ring - 1, ring))
    row0 = (0, plan.half)
    lane0 = (0, plan.rows - plan.span)

    barrier = pltpu.get_barrier_semaphore()
    for there in neighbours:
        pl.semaphore_signal(barrier, inc=1, device_id={axis: there}, device_id_type=pl.DeviceIdType.MESH)

    def chunk(d, k, scatter):
        return plan.chunk(me, d, k + jnp.where(scatter, 1, 0))

    def shared(k):
        return lax.rem(2 * k, ring) == 0

    def job_unit(d, s, k):
        return plan.unit(s, chunk(d, k, True))

    columns = plan.columns

    def block(u, d):
        m, cols = columns(u)
        return x_ref.at[m, pl.ds(row0[d], plan.half), cols]

    def a_load(m):
        return pltpu.make_async_copy(a_ref.at[0, m], a_buf.at[m % A_SLOTS], a_sem.at[m % A_SLOTS])

    def g_load(d, u, n):
        m, cols = columns(u)
        slot = lax.rem(n, G_SLOTS)
        return pltpu.make_async_copy(g_ref.at[0, m, :, cols], g_buf.at[d, slot], g_sem.at[d, slot])

    def fetch(n):
        has, s, k = plan.job(n)

        @pl.when(has)
        def _():
            g_load(0, job_unit(0, s, k), n).start()

        @pl.when(jnp.logical_and(has, jnp.logical_not(shared(k))))
        def _():
            g_load(1, job_unit(1, s, k), n).start()

    def multiply(n):
        has, s, k = plan.job(n)

        @pl.when(has)
        def _():
            for d in (0, 1):
                u = job_unit(d, s, k)
                if d == 0:
                    g_load(0, u, n).wait()
                else:

                    @pl.when(jnp.logical_not(shared(k)))
                    def _():
                        g_load(1, u, n).wait()

                from_buf = 0 if d == 0 else jnp.where(shared(k), 0, 1)
                prod[d, lax.rem(n, P_SLOTS)] = dot(
                    a_buf[lax.rem(u // plan.per_matrix, A_SLOTS), :, pl.ds(lane0[d], plan.span)],
                    g_buf[from_buf, lax.rem(n, G_SLOTS)],
                )

    piece, quick = plan.tokens // PIECES, plan.quick
    first_unit = job_unit(0, 0, 0)
    first_m = first_unit // plan.per_matrix
    other_m = 1 - first_m
    parts = (
        (0, (0, quick), (0, quick), (0, quick)),
        (1, (plan.half - quick, quick), (plan.span - quick, quick), (plan.rows - quick, quick)),
        (0, (quick, plan.half - quick), (quick, plan.span - quick), (quick, plan.span - quick)),
        (1, (0, plan.half - quick), (0, plan.span - quick), (plan.span, plan.rows - quick - plan.span)),
    )

    def first_a(p, i):
        toks, lanes = pl.ds(i * piece, piece), pl.ds(*parts[p][3])
        return pltpu.make_async_copy(
            a_ref.at[0, first_m, toks, lanes], a_buf.at[first_m, toks, lanes], first_sem.at[p, i]
        )

    def first_g(i):
        toks, (m, cols) = pl.ds(i * piece, piece), columns(first_unit)
        return pltpu.make_async_copy(g_ref.at[0, m, toks, cols], g_buf.at[0, 0, toks], first_sem.at[len(parts), i])

    def first_remote(p):
        d, (row, tall), _, _ = parts[p]
        m, cols = columns(first_unit)
        at = x_ref.at[m, pl.ds(row0[d] + row, tall), cols]
        return pltpu.make_async_remote_copy(
            src_ref=at,
            dst_ref=at,
            send_sem=first_send.at[p],
            recv_sem=first_recv.at[p],
            device_id={axis: neighbours[d]},
            device_id_type=pl.DeviceIdType.MESH,
        )

    other_a = pltpu.make_async_copy(a_ref.at[0, other_m], a_buf.at[other_m], a_sem.at[1])

    def first_part(p):
        d, (row, tall), (at, wide), _ = parts[p]
        for i in range(PIECES):
            first_a(p, i).wait()
            if p == 0:
                first_g(i).wait()
            if p + 1 < len(parts):
                first_a(p + 1, i).start()
            elif i == 0:
                other_a.start()
            toks = pl.ds(i * piece, piece)
            made = dot(a_buf[first_m, toks, pl.ds(lane0[d] + at, wide)], g_buf[0, 0, toks])
            if i == 0:
                prod[d, 0, pl.ds(at, wide), :] = made
            else:
                prod[d, 0, pl.ds(at, wide), :] += made
        m, cols = columns(first_unit)
        mine = prod[d, 0, pl.ds(row0[d] - lane0[d] + row, tall), :]
        x_ref[m, pl.ds(row0[d] + row, tall), cols] = mine.astype(x_ref.dtype)
        if p == 0:
            pl.semaphore_wait(barrier, 2)
        first_remote(p).start()

    def add_product(d, n, u, fresh):
        off = row0[d] - lane0[d]
        mine = prod[d, lax.rem(n, P_SLOTS), pl.ds(off, plan.half), :]
        m, cols = columns(u)
        there = (m, pl.ds(row0[d], plan.half), cols)

        @pl.when(fresh)
        def _():
            x_ref[there] = mine.astype(x_ref.dtype)

        @pl.when(jnp.logical_not(fresh))
        def _():
            x_ref[there] = (x_ref[there].astype(jnp.float32) + mine).astype(x_ref.dtype)

    tails = (r_ref, l_ref)

    def remote(d, u, n, there=None):
        i = lax.rem(n, SEMS)
        return pltpu.make_async_remote_copy(
            src_ref=block(u, d),
            dst_ref=block(u, d) if there is None else there,
            send_sem=send_sem.at[d, i],
            recv_sem=recv_sem.at[d, i],
            device_id={axis: neighbours[d]},
            device_id_type=pl.DeviceIdType.MESH,
        )

    def turn_one(d, n):
        s, k, scatter = plan.at(n)
        has, js, jk = plan.job(n)
        mine = [p for p in range(len(parts)) if parts[p][0] == d]

        @pl.when(n == 2)
        def _():
            for p in mine:
                first_remote(p).wait_recv()

        @pl.when(n > 2)
        def _():
            remote(d, 0, n - 2 + SEMS).wait_recv()

        @pl.when(has)
        def _():
            add_product(d, n, job_unit(d, js, jk), jk == 0)

        @pl.when(n == SEMS)
        def _():
            for p in mine:
                first_remote(p).wait_send()

        @pl.when(n > SEMS)
        def _():
            remote(d, 0, n).wait_send()

        u = plan.unit(s, chunk(d, k, scatter))

        @pl.when(n != plan.cut - 2)
        def _():
            remote(d, u, n).start()

        @pl.when(n == plan.cut - 2)
        def _():
            remote(d, u, n, tails[d]).start()

    def multiply_next(n):
        @pl.when(n == 1)
        def _():
            other_a.wait()

        for m in range(2, plan.matrices):

            @pl.when(n == plan.load_slot(m))
            def _():
                a_load(m).start()

            @pl.when(n + 1 == plan.need_slot(m))
            def _():
                a_load(m).wait()

        multiply(n + 1)

    for i in range(PIECES):
        first_a(0, i).start()
        first_g(i).start()
    for p in range(len(parts)):
        if p == 3:
            fetch(1)
        first_part(p)
    fetch(2)
    multiply_next(0)
    fetch(3)

    def body(n, _):
        for d in (0, 1):
            turn_one(d, n)
        multiply_next(n)
        fetch(n + 3)
        return 0

    slots = plan.cut
    lax.fori_loop(1, slots, body, 0)
    for n in range(slots - 2, slots):
        for d in (0, 1):
            remote(d, 0, n, tails[d] if n == slots - 2 else None).wait_recv()
    for n in range(slots - SEMS, slots):
        for d in (0, 1):
            remote(d, 0, n).wait_send()


def write_kernel(pieces, x_ref, out_ref, sem):
    matrices, rows, _ = x_ref.shape
    tall = rows // pieces
    copies = []
    for i in range(matrices * pieces):
        at = (i // pieces, pl.ds(i % pieces * tall, tall))
        copies.append(pltpu.make_async_copy(x_ref.at[at], out_ref.at[at], sem.at[i]))
    for c in copies:
        c.start()
    for c in copies:
        c.wait()


def place_kernel(plan, axis, x_ref, *refs):
    *blocks, out_ref, sem = refs
    me = lax.axis_index(axis)
    copies = []
    for i, b in enumerate(blocks):
        d, hop = i % 2, plan.ring - 2 + i // 2
        m, cols = plan.columns(plan.unit(plan.sets - 1, plan.chunk(me, d, hop)))
        copies.append(pltpu.make_async_copy(b, out_ref.at[m, pl.ds(d * plan.half, plan.half), cols], sem.at[i]))
    for c in copies:
        c.start()
    for c in copies:
        c.wait()


def solution(mesh):
    axis = "dp"

    def device(a, g):
        _, matrices, tokens, rows = a.shape
        cols = g.shape[-1]
        plan = Plan(mesh.shape[axis], matrices, tokens, rows, cols)
        block = (plan.half, COLS)
        sums, right, left = pl.pallas_call(
            functools.partial(reduce_kernel, plan, axis),
            out_shape=(
                pltpu.VMEM((matrices, rows, cols), jnp.bfloat16),
                jax.ShapeDtypeStruct(block, jnp.bfloat16),
                jax.ShapeDtypeStruct(block, jnp.bfloat16),
            ),
            in_specs=[pl.BlockSpec(memory_space=pl.ANY)] * 2,
            out_specs=(
                pl.BlockSpec(memory_space=pltpu.VMEM),
                pl.BlockSpec(memory_space=pl.ANY),
                pl.BlockSpec(memory_space=pl.ANY),
            ),
            scratch_shapes=[
                pltpu.VMEM((A_SLOTS, tokens, rows), jnp.bfloat16),
                pltpu.VMEM((2, G_SLOTS, tokens, COLS), jnp.bfloat16),
                pltpu.VMEM((2, P_SLOTS, plan.span, COLS), jnp.float32),
                pltpu.SemaphoreType.DMA((A_SLOTS,)),
                pltpu.SemaphoreType.DMA((2, G_SLOTS)),
                pltpu.SemaphoreType.DMA((2, SEMS)),
                pltpu.SemaphoreType.DMA((2, SEMS)),
                pltpu.SemaphoreType.DMA((5, PIECES)),
                pltpu.SemaphoreType.DMA((4,)),
                pltpu.SemaphoreType.DMA((4,)),
            ],
            compiler_params=pltpu.CompilerParams(
                collective_id=0, has_side_effects=True, vmem_limit_bytes=44 * 2**20
            ),
            name="ring_sums",
        )(a, g)
        ring = plan.ring
        from_left = lax.ppermute(right, axis, [(i, (i + 1) % ring) for i in range(ring)])
        from_right = lax.ppermute(left, axis, [(i, (i - 1) % ring) for i in range(ring)])
        result = jax.ShapeDtypeStruct((matrices, rows, cols), jnp.bfloat16)
        size = matrices * rows * cols * 2
        written = pl.pallas_call(
            functools.partial(write_kernel, WRITES),
            out_shape=result,
            in_specs=[pl.BlockSpec(memory_space=pltpu.VMEM)],
            out_specs=pl.BlockSpec(memory_space=pl.ANY),
            scratch_shapes=[pltpu.SemaphoreType.DMA((matrices * WRITES,))],
            compiler_params=pltpu.CompilerParams(vmem_limit_bytes=2**20),
            cost_estimate=pl.CostEstimate(flops=0, bytes_accessed=2 * size, transcendentals=0),
            name="write_sums",
        )(pltpu.with_memory_space_constraint(sums, pltpu.VMEM))
        return pl.pallas_call(
            functools.partial(place_kernel, plan, axis),
            out_shape=result,
            in_specs=[pl.BlockSpec(memory_space=pl.ANY)] + [pl.BlockSpec(memory_space=pltpu.VMEM)] * 4,
            out_specs=pl.BlockSpec(memory_space=pl.ANY),
            scratch_shapes=[pltpu.SemaphoreType.DMA((4,))],
            input_output_aliases={0: 0},
            compiler_params=pltpu.CompilerParams(vmem_limit_bytes=4 * 2**20),
            name="place_last",
        )(written, right, left, from_left, from_right)

    spec = P(("rep", axis))
    return jax.shard_map(device, mesh=mesh, in_specs=(spec, spec), out_specs=P("rep"), check_vma=False)
```

```python
import functools

import jax
import jax.numpy as jnp
from jax import lax
from jax.experimental import pallas as pl
from jax.experimental.pallas import tpu as pltpu
from jax.sharding import PartitionSpec as P

COLS = 256
LANES = 128
A_SLOTS = 3
G_SLOTS = 3
PIECES = 4
P_SLOTS = 2
SEMS = 8
WRITES = 4


def dot(a, g):
    return lax.dot_general(a, g, (((0,), (0,)), ((), ())), preferred_element_type=jnp.float32)


class Plan:
    def __init__(self, ring, matrices, tokens, rows, cols):
        self.ring, self.matrices, self.tokens, self.rows, self.cols = ring, matrices, tokens, rows, cols
        self.per_matrix = cols // COLS
        self.units = matrices * self.per_matrix
        self.sets = self.units // ring
        assert self.sets * ring == self.units and self.sets >= 3
        self.half = rows // 2
        self.span = -(-self.half // LANES) * LANES
        self.phase = 2 * (ring - 1)
        self.slots = self.sets * self.phase
        self.cut = self.slots - 1

    def unit(self, s, c):
        return s * self.ring + c

    def columns(self, u):
        j = lax.rem(u, self.per_matrix)
        return u // self.per_matrix, pl.ds(pl.multiple_of(j * COLS, COLS), COLS)

    def chunk(self, me, d, hop):
        return lax.rem(me + (self.ring - hop if d == 0 else self.ring - 2 + hop), self.ring)

    def final_slot(self, s):
        return (self.phase + 1 + 2 * s) if s < 2 else s * self.phase + 1

    def first_slot(self, s):
        return s if s < 2 else (s - 1) * self.phase

    def load_slot(self, m):
        if m < A_SLOTS:
            return m
        last = (m - A_SLOTS + 1) * self.per_matrix - 1
        return self.final_slot(last // self.ring) + 1

    def need_slot(self, m):
        return self.first_slot(m * self.per_matrix // self.ring)

    def at(self, n):
        p, q = n // self.phase, n % self.phase
        b, k = q % 2, q // 2
        first, last = p == 0, p == self.sets - 1
        s_a = jnp.where(first, 0, jnp.where(last, self.sets - 2, p + 1))
        s_b = jnp.where(first, 1, jnp.where(last, self.sets - 1, p - 1))
        s = jnp.where(b == 0, s_a, s_b)
        scatter = jnp.logical_or(first, jnp.logical_and(b == 0, jnp.logical_not(last)))
        return s, k, scatter

    def final(self, n):
        ends, which = False, 0
        for s in range(self.sets):
            hit = n == self.final_slot(s)
            ends = jnp.logical_or(ends, hit)
            which = jnp.where(hit, s, which)
        return ends, which

    def job(self, n):
        s, k, scatter = self.at(n)
        ends, which = self.final(n)
        has = jnp.logical_and(jnp.logical_or(scatter, ends), n < self.slots)
        return has, jnp.where(ends, which, s), jnp.where(ends, self.ring - 1, k)


def reduce_kernel(plan, axis, a_ref, g_ref, x_ref, r_ref, l_ref, a_buf, g_buf, prod, a_sem, g_sem, send_sem, recv_sem, first_sem):
    ring = plan.ring
    me = lax.axis_index(axis)
    neighbours = (lax.rem(me + 1, ring), lax.rem(me + ring - 1, ring))
    row0 = (0, plan.half)
    lane0 = (0, plan.rows - plan.span)

    barrier = pltpu.get_barrier_semaphore()
    for there in neighbours:
        pl.semaphore_signal(barrier, inc=1, device_id={axis: there}, device_id_type=pl.DeviceIdType.MESH)

    def chunk(d, k, scatter):
        return plan.chunk(me, d, k + jnp.where(scatter, 1, 0))

    def shared(k):
        return lax.rem(2 * k, ring) == 0

    def job_unit(d, s, k):
        return plan.unit(s, chunk(d, k, True))

    columns = plan.columns

    def block(u, d):
        m, cols = columns(u)
        return x_ref.at[m, pl.ds(row0[d], plan.half), cols]

    def a_load(m):
        return pltpu.make_async_copy(a_ref.at[0, m], a_buf.at[m % A_SLOTS], a_sem.at[m % A_SLOTS])

    def g_load(d, u, n):
        m, cols = columns(u)
        slot = lax.rem(n, G_SLOTS)
        return pltpu.make_async_copy(g_ref.at[0, m, :, cols], g_buf.at[d, slot], g_sem.at[d, slot])

    def fetch(n):
        has, s, k = plan.job(n)

        @pl.when(has)
        def _():
            g_load(0, job_unit(0, s, k), n).start()

        @pl.when(jnp.logical_and(has, jnp.logical_not(shared(k))))
        def _():
            g_load(1, job_unit(1, s, k), n).start()

    def multiply(n):
        has, s, k = plan.job(n)

        @pl.when(has)
        def _():
            for d in (0, 1):
                u = job_unit(d, s, k)
                if d == 0:
                    g_load(0, u, n).wait()
                else:

                    @pl.when(jnp.logical_not(shared(k)))
                    def _():
                        g_load(1, u, n).wait()

                from_buf = 0 if d == 0 else jnp.where(shared(k), 0, 1)
                prod[d, lax.rem(n, P_SLOTS)] = dot(
                    a_buf[lax.rem(u // plan.per_matrix, A_SLOTS), :, pl.ds(lane0[d], plan.span)],
                    g_buf[from_buf, lax.rem(n, G_SLOTS)],
                )

    piece = plan.tokens // PIECES
    splits = ((0, plan.span), (plan.span, plan.rows - plan.span))

    def first_a(d, i):
        toks, lanes = pl.ds(i * piece, piece), pl.ds(*splits[d])
        return pltpu.make_async_copy(a_ref.at[0, 0, toks, lanes], a_buf.at[0, toks, lanes], first_sem.at[d, i])

    def first_g(i):
        toks, (m, cols) = pl.ds(i * piece, piece), columns(job_unit(0, 0, 0))
        return pltpu.make_async_copy(g_ref.at[0, m, toks, cols], g_buf.at[0, 0, toks], first_sem.at[2, i])

    def first_product(d):
        for i in range(PIECES):
            first_a(d, i).wait()
            if d == 0:
                first_g(i).wait()
            toks = pl.ds(i * piece, piece)
            part = dot(a_buf[0, toks, pl.ds(lane0[d], plan.span)], g_buf[0, 0, toks])
            if i == 0:
                prod[d, 0] = part
            else:
                prod[d, 0] += part

    def add_product(d, n, u, fresh):
        off = row0[d] - lane0[d]
        mine = prod[d, lax.rem(n, P_SLOTS), pl.ds(off, plan.half), :]
        m, cols = columns(u)
        there = (m, pl.ds(row0[d], plan.half), cols)

        if fresh is True:
            x_ref[there] = mine.astype(x_ref.dtype)
            return

        @pl.when(fresh)
        def _():
            x_ref[there] = mine.astype(x_ref.dtype)

        @pl.when(jnp.logical_not(fresh))
        def _():
            x_ref[there] = (x_ref[there].astype(jnp.float32) + mine).astype(x_ref.dtype)

    tails = (r_ref, l_ref)

    def remote(d, u, n, there=None):
        i = lax.rem(n, SEMS)
        return pltpu.make_async_remote_copy(
            src_ref=block(u, d),
            dst_ref=block(u, d) if there is None else there,
            send_sem=send_sem.at[d, i],
            recv_sem=recv_sem.at[d, i],
            device_id={axis: neighbours[d]},
            device_id_type=pl.DeviceIdType.MESH,
        )

    def turn_one(d, n):
        s, k, scatter = plan.at(n)
        has, js, jk = plan.job(n)

        @pl.when(n >= 2)
        def _():
            remote(d, 0, n - 2 + SEMS).wait_recv()

        @pl.when(has)
        def _():
            add_product(d, n, job_unit(d, js, jk), jk == 0)

        @pl.when(n >= SEMS)
        def _():
            remote(d, 0, n).wait_send()

        u = plan.unit(s, chunk(d, k, scatter))

        @pl.when(n != plan.cut - 2)
        def _():
            remote(d, u, n).start()

        @pl.when(n == plan.cut - 2)
        def _():
            remote(d, u, n, tails[d]).start()

    def first_turn(d):
        u = job_unit(d, 0, 0)
        add_product(d, 0, u, True)
        remote(d, u, 0).start()

    def multiply_next(n):
        for m in range(1, plan.matrices):
            if m >= 2:

                @pl.when(n == plan.load_slot(m))
                def _():
                    a_load(m).start()

            @pl.when(n + 1 == plan.need_slot(m))
            def _():
                a_load(m).wait()

        multiply(n + 1)

    for i in range(PIECES):
        first_a(0, i).start()
        first_g(i).start()
    for i in range(PIECES):
        first_a(1, i).start()
    fetch(1)
    if plan.matrices > 1:
        a_load(1).start()
    fetch(2)
    first_product(0)
    pl.semaphore_wait(barrier, 2)
    first_turn(0)
    first_product(1)
    first_turn(1)
    multiply_next(0)
    fetch(3)

    def body(n, _):
        for d in (0, 1):
            turn_one(d, n)
        multiply_next(n)
        fetch(n + 3)
        return 0

    slots = plan.cut
    lax.fori_loop(1, slots, body, 0)
    for n in range(slots - 2, slots):
        for d in (0, 1):
            remote(d, 0, n, tails[d] if n == slots - 2 else None).wait_recv()
    for n in range(slots - SEMS, slots):
        for d in (0, 1):
            remote(d, 0, n).wait_send()


def write_kernel(pieces, x_ref, out_ref, sem):
    matrices, rows, _ = x_ref.shape
    tall = rows // pieces
    copies = []
    for i in range(matrices * pieces):
        at = (i // pieces, pl.ds(i % pieces * tall, tall))
        copies.append(pltpu.make_async_copy(x_ref.at[at], out_ref.at[at], sem.at[i]))
    for c in copies:
        c.start()
    for c in copies:
        c.wait()


def place_kernel(plan, axis, x_ref, *refs):
    *blocks, out_ref, sem = refs
    me = lax.axis_index(axis)
    copies = []
    for i, b in enumerate(blocks):
        d, hop = i % 2, plan.ring - 2 + i // 2
        m, cols = plan.columns(plan.unit(plan.sets - 1, plan.chunk(me, d, hop)))
        copies.append(pltpu.make_async_copy(b, out_ref.at[m, pl.ds(d * plan.half, plan.half), cols], sem.at[i]))
    for c in copies:
        c.start()
    for c in copies:
        c.wait()


def solution(mesh):
    axis = "dp"

    def device(a, g):
        _, matrices, tokens, rows = a.shape
        cols = g.shape[-1]
        plan = Plan(mesh.shape[axis], matrices, tokens, rows, cols)
        block = (plan.half, COLS)
        sums, right, left = pl.pallas_call(
            functools.partial(reduce_kernel, plan, axis),
            out_shape=(
                pltpu.VMEM((matrices, rows, cols), jnp.bfloat16),
                jax.ShapeDtypeStruct(block, jnp.bfloat16),
                jax.ShapeDtypeStruct(block, jnp.bfloat16),
            ),
            in_specs=[pl.BlockSpec(memory_space=pl.ANY)] * 2,
            out_specs=(
                pl.BlockSpec(memory_space=pltpu.VMEM),
                pl.BlockSpec(memory_space=pl.ANY),
                pl.BlockSpec(memory_space=pl.ANY),
            ),
            scratch_shapes=[
                pltpu.VMEM((A_SLOTS, tokens, rows), jnp.bfloat16),
                pltpu.VMEM((2, G_SLOTS, tokens, COLS), jnp.bfloat16),
                pltpu.VMEM((2, P_SLOTS, plan.span, COLS), jnp.float32),
                pltpu.SemaphoreType.DMA((A_SLOTS,)),
                pltpu.SemaphoreType.DMA((2, G_SLOTS)),
                pltpu.SemaphoreType.DMA((2, SEMS)),
                pltpu.SemaphoreType.DMA((2, SEMS)),
                pltpu.SemaphoreType.DMA((3, PIECES)),
            ],
            compiler_params=pltpu.CompilerParams(
                collective_id=0, has_side_effects=True, vmem_limit_bytes=44 * 2**20
            ),
            name="ring_sums",
        )(a, g)
        ring = plan.ring
        from_left = lax.ppermute(right, axis, [(i, (i + 1) % ring) for i in range(ring)])
        from_right = lax.ppermute(left, axis, [(i, (i - 1) % ring) for i in range(ring)])
        result = jax.ShapeDtypeStruct((matrices, rows, cols), jnp.bfloat16)
        size = matrices * rows * cols * 2
        written = pl.pallas_call(
            functools.partial(write_kernel, WRITES),
            out_shape=result,
            in_specs=[pl.BlockSpec(memory_space=pltpu.VMEM)],
            out_specs=pl.BlockSpec(memory_space=pl.ANY),
            scratch_shapes=[pltpu.SemaphoreType.DMA((matrices * WRITES,))],
            compiler_params=pltpu.CompilerParams(vmem_limit_bytes=2**20),
            cost_estimate=pl.CostEstimate(flops=0, bytes_accessed=2 * size, transcendentals=0),
            name="write_sums",
        )(pltpu.with_memory_space_constraint(sums, pltpu.VMEM))
        return pl.pallas_call(
            functools.partial(place_kernel, plan, axis),
            out_shape=result,
            in_specs=[pl.BlockSpec(memory_space=pl.ANY)] + [pl.BlockSpec(memory_space=pltpu.VMEM)] * 4,
            out_specs=pl.BlockSpec(memory_space=pl.ANY),
            scratch_shapes=[pltpu.SemaphoreType.DMA((4,))],
            input_output_aliases={0: 0},
            compiler_params=pltpu.CompilerParams(vmem_limit_bytes=4 * 2**20),
            name="place_last",
        )(written, right, left, from_left, from_right)

    spec = P(("rep", axis))
    return jax.shard_map(device, mesh=mesh, in_specs=(spec, spec), out_specs=P("rep"), check_vma=False)
```
